8 devices in a mesh: data: 1 (over z), fsdp: 2 (over y), tp: 4 (over x, core).
Axes of the slice: x: 2, y: 2, z: 1, core: 2. Of those that a mesh axis runs over, the one named last changes fastest.
Arguments:
- hidden: bfloat16 [16384, 5120], P(('data', 'fsdp', 'tp'))
- ln_scale: float32 [5120], replicated
- w_in: bfloat16 [5120, 13824], P('fsdp', 'tp')
- w_out: bfloat16 [13824, 5120], P(('tp', 'fsdp'))
Outputs:
- output: bfloat16 [16384, 5120], P(('data', 'fsdp', 'tp'))
All inputs are finite; a program needn't handle non-finite values.
Results may differ from the reference program's by a relative error of at most 0.001.
Values are sent between devices in bfloat16 or wider.
A program may use at most 1 GiB of HBM per device.

```python
import jax
import jax.numpy as jnp
from jax import lax

TOKENS_DEV = 2048
MODEL_DIM = 5120
FFN_DIM = 13824
GROUP_DEVICES = 8
GROUP_ROWS = GROUP_DEVICES * TOKENS_DEV
LN_EPS = 1e-6


def setup_inputs(seed: int = 0, part: int = 0) -> dict:
    base_key = jax.random.key(seed)
    key_rows, key_gain, key_in, key_out = jax.random.split(base_key, 4)
    key_rows = jax.random.fold_in(key_rows, part)
    hidden = jax.random.normal(key_rows, (GROUP_ROWS, MODEL_DIM), jnp.float32).astype(jnp.bfloat16)
    ln_scale = 1.0 + 0.3 * jax.random.normal(key_gain, (MODEL_DIM,), jnp.float32)
    w_in = (jax.random.normal(key_in, (MODEL_DIM, FFN_DIM), jnp.float32) * MODEL_DIM ** -0.5).astype(jnp.bfloat16)
    w_out = (jax.random.normal(key_out, (FFN_DIM, MODEL_DIM), jnp.float32) * (1.5 * FFN_DIM ** -0.5)).astype(jnp.bfloat16)
    return {"hidden": hidden, "ln_scale": ln_scale, "w_in": w_in, "w_out": w_out}


def layer_norm(row_block, ln_scale):
    block_f32 = row_block.astype(jnp.float32)
    centered = block_f32 - jnp.mean(block_f32, axis=-1, keepdims=True)
    var_row = jnp.mean(centered * centered, axis=-1, keepdims=True)
    return (centered * lax.rsqrt(var_row + LN_EPS) * ln_scale).astype(jnp.bfloat16)


def reference(hidden, ln_scale, w_in, w_out):
    normed = layer_norm(hidden, ln_scale).reshape(GROUP_DEVICES, TOKENS_DEV, MODEL_DIM)

    def mlp_block(row_block):
        pre_act = jnp.dot(row_block, w_in, preferred_element_type=jnp.float32)
        act_out = jax.nn.gelu(pre_act, approximate=True).astype(jnp.bfloat16)
        return jnp.dot(act_out, w_out, preferred_element_type=jnp.float32)

    mlp_out = lax.map(mlp_block, normed).reshape(GROUP_ROWS, MODEL_DIM)
    return (hidden.astype(jnp.float32) + mlp_out).astype(jnp.bfloat16)
```

```python
import jax
import jax.numpy as jnp
from jax import lax
from jax.experimental import pallas as pl
from jax.experimental.pallas import tpu as pltpu
from jax.sharding import PartitionSpec as P

LN_EPS = 1e-6
MESH = pl.DeviceIdType.MESH

ROWS, DIM, FFN = 2048, 5120, 13824
K_PIECE, F_BLOCK = 2560, 3456
F_PIECE = 1728
CA, NA = 128, 27
CB, NB = 256, 20
S = NA + NB
LEAD = 2
TM = 256
MT = ROWS // TM
NPAIR = 8


def kernel(hid, gain, w_in, w_out, out, g1, g2, hbm_h,
           r_x, r_y, r_dx, r_dy, r_c, s_sem, ld_sem, t_sem, o_sem):
    f = lax.axis_index("fsdp")
    t = lax.axis_index("tp")
    x, k = t // 2, t % 2
    xn = {"tp": 2 * (1 - x) + k}
    yn = {"fsdp": 1 - f}
    cn = {"tp": 2 * x + 1 - k}
    me = (f, x, k)
    px, py, pd = (f, 1 - x, k), (1 - f, x, k), (1 - f, 1 - x, k)

    def piece_a(i, who, half=None):
        wf, wx, wk = who
        n = K_PIECE if half is None else K_PIECE // 2
        r0 = wf * K_PIECE + (0 if half is None else half * n)
        return g1.at[i, pl.ds(pl.multiple_of(r0, 128), n),
                     pl.ds(pl.multiple_of((2 * wx + wk) * CA, 128), CA)]

    def piece_b(j, who, half=None):
        wf, wx, wk = who
        n = F_PIECE if half is None else F_PIECE // 2
        r0 = (2 * wx + wk) * F_BLOCK + wf * F_PIECE + (0 if half is None else half * n)
        return g2.at[pl.ds(pl.multiple_of(r0, 32), n),
                     pl.ds(pl.multiple_of(j * CB, 128), CB)]

    def own_a(i):
        return w_in.at[:, pl.ds(pl.multiple_of(i * CA, 128), CA)]

    def own_b(j):
        return w_out.at[:, pl.ds(pl.multiple_of(j * CB, 128), CB)]

    def rc(src, dst, kind, ph, recv, dev):
        return pltpu.make_async_remote_copy(
            src, dst, s_sem.at[ph, kind], recv, device_id=dev, device_id_type=MESH)

    phases = ((0, piece_a, own_a, 0, NA), (1, piece_b, own_b, NA, S))

    def each_phase(i, body):
        if isinstance(i, int):
            for ph, piece, own, lo, hi in phases:
                if lo <= i < hi:
                    body(ph, piece, own, i - lo)
            return
        for ph, piece, own, lo, hi in phases:
            pl.when(jnp.logical_and(i >= lo, i < hi))(
                lambda ph=ph, piece=piece, own=own, lo=lo: body(ph, piece, own, i - lo))

    def send_own(i):
        def body(ph, piece, own, n):
            rc(own(n), piece(n, me), 0, ph, r_x.at[i], xn).start()
            rc(own(n), piece(n, me), 1, ph, r_y.at[i], yn).start()
            rc(own(n), piece(n, me), 2, ph, r_c.at[i], cn).start()
        each_phase(i, body)

    def comm_point(i):
        def body(ph, piece, own, n):
            rc(own(n), piece(n, px), 0, ph, r_x.at[i], xn).wait_recv()
            rc(piece(n, px, 0), piece(n, px, 0), 3, ph, r_dy.at[i], yn).start()
            rc(own(n), piece(n, py), 1, ph, r_y.at[i], yn).wait_recv()
            rc(piece(n, py, 1), piece(n, py, 1), 4, ph, r_dx.at[i], xn).start()
            rc(piece(n, px), piece(n, px), 5, ph, r_c.at[i], cn).start()
            rc(piece(n, py), piece(n, py), 6, ph, r_c.at[i], cn).start()
        each_phase(i, body)
        send_own(i + LEAD)

    def d_point(i):
        def body(ph, piece, own, n):
            rc(piece(n, pd, 0), piece(n, pd, 0), 3, ph, r_dy.at[i], yn).wait_recv()
            rc(piece(n, pd, 0), piece(n, pd, 0), 7, ph, r_c.at[i], cn).start()
            rc(piece(n, pd, 1), piece(n, pd, 1), 4, ph, r_dx.at[i], xn).wait_recv()
            rc(piece(n, pd, 1), piece(n, pd, 1), 8, ph, r_c.at[i], cn).start()
        each_phase(i, body)

    def c_wait(i):
        def body(ph, piece, own, n):
            whole = (g1.at[n, :, pl.ds(0, 2 * CA)] if ph == 0
                     else g2.at[pl.ds(0, 4 * F_PIECE), pl.ds(0, CB)])
            pltpu.make_async_copy(whole, whole, r_c.at[i]).wait()
        each_phase(i, body)

    others = [(a, b, c) for a in (0, 1) for b in (0, 1) for c in (0, 1)][1:]

    def who(d):
        a, b, c = d
        return (1 - f if a else f, 1 - x if b else x, 1 - k if c else k)

    barrier = pltpu.get_barrier_semaphore()
    for nb in (xn, yn, cn):
        pl.semaphore_signal(barrier, inc=1, device_id=nb, device_id_type=MESH)
    pl.semaphore_wait(barrier, 3)
    for i in range(LEAD):
        send_own(i)

    def phase_a(u, w_buf, stage, h_stage, gain_v):
        pltpu.make_async_copy(gain, gain_v, t_sem.at[0]).start()

        def load_rows(m):
            return pltpu.make_async_copy(
                hid.at[pl.ds(m * TM, TM)], stage.at[m % 2], o_sem.at[m % 2, 0])

        load_rows(0).start()
        pltpu.make_async_copy(gain, gain_v, t_sem.at[0]).wait()

        @pl.loop(0, MT)
        def _(m):
            pl.when(m + 1 < MT)(lambda: load_rows(m + 1).start())
            load_rows(m).wait()

            @pl.loop(0, TM // 32)
            def _(r):
                rows = pl.ds(pl.multiple_of(r * 32, 32), 32)
                v = stage[m % 2, rows, :].astype(jnp.float32)
                cen = v - jnp.mean(v, axis=-1, keepdims=True)
                var = jnp.mean(cen * cen, axis=-1, keepdims=True)
                res = cen * lax.rsqrt(var + LN_EPS) * gain_v[...]
                u[pl.ds(pl.multiple_of(m * TM + r * 32, 32), 32), :] = res.astype(jnp.bfloat16)

        def load_w(a):
            slot = a % 2
            for d in others:
                wf, wx, wk = who(d)
                pltpu.make_async_copy(
                    piece_a(a, (wf, wx, wk)),
                    w_buf.at[slot, pl.ds(pl.multiple_of(wf * K_PIECE, 128), K_PIECE),
                             pl.ds(pl.multiple_of((2 * wx + wk) * CA, 128), CA)],
                    ld_sem.at[slot]).start()
            pltpu.make_async_copy(
                own_a(a),
                w_buf.at[slot, pl.ds(pl.multiple_of(f * K_PIECE, 128), K_PIECE),
                         pl.ds(pl.multiple_of(t * CA, 128), CA)],
                ld_sem.at[slot]).start()

        def wait_w(a):
            pltpu.make_async_copy(g1.at[0], w_buf.at[a % 2], ld_sem.at[a % 2]).wait()

        def h_copies(a, m):
            return [pltpu.make_async_copy(
                h_stage.at[m % 2, :, pl.ds(q * CA, CA)],
                hbm_h.at[pl.ds(m * TM, TM), pl.ds(pl.multiple_of(q * F_BLOCK + a * CA, 128), CA)],
                o_sem.at[m % 2, q]) for q in range(4)]

        comm_point(0)

        @pl.loop(0, NA + 1)
        def _(i):
            comm_point(i + 1)
            pl.when(i < NA)(lambda: d_point(i))
            a = i - 1

            @pl.when(i == 0)
            def _():
                c_wait(i)
                load_w(i)

            @pl.when(i > 0)
            def _():
                wait_w(a)

                @pl.loop(0, MT)
                def _(m):
                    @pl.when(jnp.logical_and(m == 2, i < NA))
                    def _():
                        c_wait(i)
                        load_w(i)

                    pre = jnp.dot(u[pl.ds(pl.multiple_of(m * TM, TM), TM), :], w_buf[a % 2],
                                  preferred_element_type=jnp.float32)
                    cdf = 0.5 * (1.0 + jnp.tanh(0.7978845608028654 * (pre + 0.044715 * (pre * pre * pre))))
                    act = (pre * cdf).astype(jnp.bfloat16)

                    @pl.when(jnp.logical_or(a > 0, m >= 2))
                    def _():
                        for c in h_copies(a, m):
                            c.wait()

                    h_stage[m % 2] = act
                    for c in h_copies(a, m):
                        c.start()

        for m in (0, 1):
            for c in h_copies(NA - 1, m):
                c.wait()

    pl.run_scoped(
        phase_a,
        pltpu.VMEM((ROWS, DIM), jnp.bfloat16),
        pltpu.VMEM((2, DIM, 4 * CA), jnp.bfloat16),
        pltpu.VMEM((2, TM, DIM), jnp.bfloat16),
        pltpu.VMEM((2, TM, 4 * CA), jnp.bfloat16),
        pltpu.VMEM((1, DIM), jnp.float32),
    )

    def phase_b(w_buf, h_buf, x_buf, y_buf):
        def load_w(j):
            slot = j % 4
            for d in others:
                wf, wx, wk = who(d)
                r0 = (2 * wx + wk) * F_BLOCK + wf * F_PIECE
                pltpu.make_async_copy(
                    piece_b(j, (wf, wx, wk)),
                    w_buf.at[slot, pl.ds(pl.multiple_of(r0, 32), F_PIECE), :],
                    ld_sem.at[slot]).start()
            r0 = t * F_BLOCK + f * F_PIECE
            pltpu.make_async_copy(
                own_b(j), w_buf.at[slot, pl.ds(pl.multiple_of(r0, 32), F_PIECE), :],
                ld_sem.at[slot]).start()

        def wait_w(j):
            pltpu.make_async_copy(
                g2.at[:, pl.ds(0, CB)], w_buf.at[j % 4], ld_sem.at[j % 4]).wait()

        def load_h(m, slot):
            return pltpu.make_async_copy(
                hbm_h.at[pl.ds(pl.multiple_of(m * TM, TM), TM)], h_buf.at[slot], t_sem.at[slot])

        def load_x(m, j, n, slot):
            return pltpu.make_async_copy(
                hid.at[pl.ds(pl.multiple_of(m * TM, TM), TM),
                       pl.ds(pl.multiple_of(j * CB, 128), n * CB)],
                x_buf.at[slot, :, pl.ds(0, n * CB)], t_sem.at[2 + slot])

        def store_y(m, j, n, slot):
            return pltpu.make_async_copy(
                y_buf.at[slot, :, pl.ds(0, n * CB)],
                out.at[pl.ds(pl.multiple_of(m * TM, TM), TM),
                       pl.ds(pl.multiple_of(j * CB, 128), n * CB)],
                o_sem.at[slot, 0])

        def compute(j, n, hooks):
            for q in range(n):
                wait_w(j + q)
            load_h(0, 0).start()
            load_x(0, j, n, 0).start()

            @pl.loop(0, MT)
            def _(m):
                slot = m % 2

                @pl.when(m + 1 < MT)
                def _():
                    load_h(m + 1, 1 - slot).start()
                    load_x(m + 1, j, n, 1 - slot).start()

                for at, hook in hooks.items():
                    pl.when(m == at)(hook)
                load_h(m, slot).wait()
                load_x(m, j, n, slot).wait()

                @pl.when(m >= 2)
                def _():
                    store_y(m, j, n, slot).wait()

                for q in range(n):
                    cols = slice(q * CB, (q + 1) * CB)
                    acc = jnp.dot(h_buf[slot], w_buf[(j + q) % 4],
                                  preferred_element_type=jnp.float32)
                    y_buf[slot, :, cols] = (
                        x_buf[slot, :, cols].astype(jnp.float32) + acc).astype(jnp.bfloat16)
                store_y(m, j, n, slot).start()

            for m in (MT - 2, MT - 1):
                store_y(m, j, n, m % 2).wait()

        d_point(NA)
        comm_point(NA + 2)
        d_point(NA + 1)
        for n in (0, 1):
            c_wait(NA + n)
            load_w(n)

        @pl.loop(1, NPAIR + 1)
        def _(p):
            j = 2 * p
            comm_point(NA + j + 1)
            d_point(NA + j)

            def mid():
                comm_point(NA + j + 2)
                d_point(NA + j + 1)

            def load():
                for q in (0, 1):
                    c_wait(NA + j + q)
                    load_w(j + q)

            compute(j - 2, 2, {3: mid, 5: load})

        j = 2 * NPAIR

        def next_comm():
            comm_point(NA + j + 3)
            d_point(NA + j + 2)

        def next_load():
            c_wait(NA + j + 2)
            load_w(j + 2)

        def last_d():
            d_point(NA + j + 3)

        def last_load():
            c_wait(NA + j + 3)
            load_w(j + 3)

        compute(j, 1, {})
        compute(j + 1, 1, {0: next_comm, 2: next_load})
        compute(j + 2, 1, {2: last_d, 3: last_load})
        compute(j + 3, 1, {})

    pl.run_scoped(
        phase_b,
        pltpu.VMEM((4, FFN, CB), jnp.bfloat16),
        pltpu.VMEM((2, TM, FFN), jnp.bfloat16),
        pltpu.VMEM((2, TM, 2 * CB), jnp.bfloat16),
        pltpu.VMEM((2, TM, 2 * CB), jnp.bfloat16),
    )

    for kind in range(9):
        rows_a = K_PIECE if kind in (0, 1, 2, 5, 6) else K_PIECE // 2
        pltpu.make_async_copy(w_in.at[pl.ds(0, rows_a)], w_in.at[pl.ds(0, rows_a)],
                              s_sem.at[0, kind]).wait()
        rows_b = F_PIECE if kind in (0, 1, 2, 5, 6) else F_PIECE // 2
        pltpu.make_async_copy(w_out.at[pl.ds(0, rows_b)], w_out.at[pl.ds(0, rows_b)],
                              s_sem.at[1, kind]).wait()


def solution(mesh):
    def local_mlp(hidden, ln_scale, w_in, w_out):
        bf16 = jnp.bfloat16
        y, _, _, _ = pl.pallas_call(
            kernel,
            out_shape=[
                jax.ShapeDtypeStruct((ROWS, DIM), bf16),
                jax.ShapeDtypeStruct((NA, DIM, 4 * CA), bf16),
                jax.ShapeDtypeStruct((FFN, DIM), bf16),
                jax.ShapeDtypeStruct((ROWS, FFN), bf16),
            ],
            in_specs=[pl.BlockSpec(memory_space=pl.ANY)] * 4,
            out_specs=[pl.BlockSpec(memory_space=pl.ANY)] * 4,
            scratch_shapes=[
                pltpu.SemaphoreType.DMA((S,)),
                pltpu.SemaphoreType.DMA((S,)),
                pltpu.SemaphoreType.DMA((S,)),
                pltpu.SemaphoreType.DMA((S,)),
                pltpu.SemaphoreType.DMA((S,)),
                pltpu.SemaphoreType.DMA((2, 9)),
                pltpu.SemaphoreType.DMA((4,)),
                pltpu.SemaphoreType.DMA((4,)),
                pltpu.SemaphoreType.DMA((2, 4)),
            ],
            compiler_params=pltpu.CompilerParams(
                collective_id=0, has_side_effects=True, vmem_limit_bytes=60 * 2**20),
            name="mlp",
        )(hidden, ln_scale.reshape(1, DIM), w_in, w_out)
        return y

    return jax.shard_map(
        local_mlp,
        mesh=mesh,
        in_specs=(P(("data", "fsdp", "tp"), None), P(None), P("fsdp", "tp"), P(("tp", "fsdp"), None)),
        out_specs=P(("data", "fsdp", "tp"), None),
        check_vma=False,
    )
```

```python
import jax
import jax.numpy as jnp
from jax import lax
from jax.experimental import pallas as pl
from jax.experimental.pallas import tpu as pltpu
from jax.sharding import PartitionSpec as P

LN_EPS = 1e-6
MESH = pl.DeviceIdType.MESH

ROWS, DIM, FFN = 2048, 5120, 13824
K_PIECE, F_BLOCK = 2560, 3456
F_PIECE = 1728
CA, NA = 128, 27
CB, NB = 256, 20
S = NA + NB
LEAD = 2
TM = 256
MT = ROWS // TM
WS = 3
RES = 1


def kernel(hid, gain, w_in, w_out, out, g1, g2, hbm_h,
           r_x, r_y, r_dx, r_dy, r_c, r_cd, s_sem, ld_sem, ld2_sem, t_sem, x_sem, o_sem):
    f = lax.axis_index("fsdp")
    t = lax.axis_index("tp")
    x, k = t // 2, t % 2
    xn = {"tp": 2 * (1 - x) + k}
    yn = {"fsdp": 1 - f}
    cn = {"tp": 2 * x + 1 - k}
    me = (f, x, k)
    px, py, pd = (f, 1 - x, k), (1 - f, x, k), (1 - f, 1 - x, k)

    def piece_a(i, who, half=None):
        wf, wx, wk = who
        n = K_PIECE if half is None else K_PIECE // 2
        r0 = wf * K_PIECE + (0 if half is None else half * n)
        return g1.at[i, pl.ds(pl.multiple_of(r0, 128), n),
                     pl.ds(pl.multiple_of((2 * wx + wk) * CA, 128), CA)]

    def piece_b(j, who, half=None):
        wf, wx, wk = who
        n = F_PIECE if half is None else F_PIECE // 2
        r0 = (2 * wx + wk) * F_BLOCK + wf * F_PIECE + (0 if half is None else half * n)
        return g2.at[pl.ds(pl.multiple_of(r0, 32), n),
                     pl.ds(pl.multiple_of(j * CB, 128), CB)]

    def own_a(i):
        return w_in.at[:, pl.ds(pl.multiple_of(i * CA, 128), CA)]

    def own_b(j):
        return w_out.at[:, pl.ds(pl.multiple_of(j * CB, 128), CB)]

    def rc(src, dst, kind, ph, recv, dev):
        return pltpu.make_async_remote_copy(
            src, dst, s_sem.at[ph, kind], recv, device_id=dev, device_id_type=MESH)

    phases = ((0, piece_a, own_a, 0, NA), (1, piece_b, own_b, NA, S))

    def each_phase(i, body):
        if isinstance(i, int):
            for ph, piece, own, lo, hi in phases:
                if lo <= i < hi:
                    body(ph, piece, own, i - lo)
            return
        for ph, piece, own, lo, hi in phases:
            pl.when(jnp.logical_and(i >= lo, i < hi))(
                lambda ph=ph, piece=piece, own=own, lo=lo: body(ph, piece, own, i - lo))

    def send_own(i):
        def body(ph, piece, own, n):
            rc(own(n), piece(n, me), 0, ph, r_x.at[i], xn).start()
            rc(own(n), piece(n, me), 1, ph, r_y.at[i], yn).start()
            rc(own(n), piece(n, me), 2, ph, r_c.at[i], cn).start()
        each_phase(i, body)

    def comm_point(i):
        def body(ph, piece, own, n):
            rc(own(n), piece(n, px), 0, ph, r_x.at[i], xn).wait_recv()
            rc(piece(n, px, 0), piece(n, px, 0), 3, ph, r_dy.at[i], yn).start()
            rc(own(n), piece(n, py), 1, ph, r_y.at[i], yn).wait_recv()
            rc(piece(n, py, 1), piece(n, py, 1), 4, ph, r_dx.at[i], xn).start()
            rc(piece(n, px), piece(n, px), 5, ph, r_c.at[i], cn).start()
            rc(piece(n, py), piece(n, py), 6, ph, r_c.at[i], cn).start()
        each_phase(i, body)
        send_own(i + LEAD)

    def d_point(i):
        def body(ph, piece, own, n):
            rc(piece(n, pd, 0), piece(n, pd, 0), 3, ph, r_dy.at[i], yn).wait_recv()
            rc(piece(n, pd, 0), piece(n, pd, 0), 7, ph, r_cd.at[i], cn).start()
            rc(piece(n, pd, 1), piece(n, pd, 1), 4, ph, r_dx.at[i], xn).wait_recv()
            rc(piece(n, pd, 1), piece(n, pd, 1), 8, ph, r_cd.at[i], cn).start()
        each_phase(i, body)

    def c_wait(i):
        def body(ph, piece, own, n):
            whole = (g1.at[n, pl.ds(0, 3 * K_PIECE // 2), pl.ds(0, 2 * CA)] if ph == 0
                     else g2.at[pl.ds(0, 3 * F_PIECE), pl.ds(0, CB)])
            pltpu.make_async_copy(whole, whole, r_c.at[i]).wait()
        each_phase(i, body)

    def cd_wait(i):
        def body(ph, piece, own, n):
            whole = (g1.at[n, pl.ds(0, K_PIECE // 2), pl.ds(0, 2 * CA)] if ph == 0
                     else g2.at[pl.ds(0, F_PIECE), pl.ds(0, CB)])
            pltpu.make_async_copy(whole, whole, r_cd.at[i]).wait()
        each_phase(i, body)

    others = [(a, b, c) for a in (0, 1) for b in (0, 1) for c in (0, 1)][1:]

    def who(d):
        a, b, c = d
        return (1 - f if a else f, 1 - x if b else x, 1 - k if c else k)

    barrier = pltpu.get_barrier_semaphore()
    for nb in (xn, yn, cn):
        pl.semaphore_signal(barrier, inc=1, device_id=nb, device_id_type=MESH)
    pl.semaphore_wait(barrier, 3)
    for i in range(LEAD):
        send_own(i)

    def phase_a(u, w_buf, stage, h_stage, gain_v):
        pltpu.make_async_copy(gain, gain_v, x_sem.at[0]).start()

        def load_rows(m):
            return pltpu.make_async_copy(
                hid.at[pl.ds(m * TM, TM)], stage.at[m % 2], o_sem.at[m % 2, 0])

        load_rows(0).start()
        pltpu.make_async_copy(gain, gain_v, x_sem.at[0]).wait()

        @pl.loop(0, MT)
        def _(m):
            pl.when(m + 1 < MT)(lambda: load_rows(m + 1).start())
            load_rows(m).wait()

            @pl.loop(0, TM // 32)
            def _(r):
                rows = pl.ds(pl.multiple_of(r * 32, 32), 32)
                v = stage[m % 2, rows, :].astype(jnp.float32)
                cen = v - jnp.mean(v, axis=-1, keepdims=True)
                var = jnp.mean(cen * cen, axis=-1, keepdims=True)
                res = cen * lax.rsqrt(var + LN_EPS) * gain_v[...]
                u[pl.ds(pl.multiple_of(m * TM + r * 32, 32), 32), :] = res.astype(jnp.bfloat16)

        def load_w(a):
            slot = a % 2
            for d in others:
                wf, wx, wk = who(d)
                pltpu.make_async_copy(
                    piece_a(a, (wf, wx, wk)),
                    w_buf.at[slot, pl.ds(pl.multiple_of(wf * K_PIECE, 128), K_PIECE),
                             pl.ds(pl.multiple_of((2 * wx + wk) * CA, 128), CA)],
                    ld_sem.at[slot]).start()
            pltpu.make_async_copy(
                own_a(a),
                w_buf.at[slot, pl.ds(pl.multiple_of(f * K_PIECE, 128), K_PIECE),
                         pl.ds(pl.multiple_of(t * CA, 128), CA)],
                ld_sem.at[slot]).start()

        def wait_w(a):
            pltpu.make_async_copy(g1.at[0], w_buf.at[a % 2], ld_sem.at[a % 2]).wait()

        def h_copies(a, m):
            return [pltpu.make_async_copy(
                h_stage.at[m % 2, :, pl.ds(q * CA, CA)],
                hbm_h.at[pl.ds(m * TM, TM), pl.ds(pl.multiple_of(q * F_BLOCK + a * CA, 128), CA)],
                o_sem.at[m % 2, q]) for q in range(4)]

        comm_point(0)

        @pl.loop(0, NA + 1)
        def _(i):
            comm_point(i + 1)
            pl.when(i < NA)(lambda: d_point(i))
            a = i - 1

            @pl.when(i == 0)
            def _():
                c_wait(i)
                cd_wait(i)
                load_w(i)

            @pl.when(i > 0)
            def _():
                wait_w(a)

                @pl.loop(0, MT)
                def _(m):
                    @pl.when(jnp.logical_and(m == 2, i < NA))
                    def _():
                        c_wait(i)
                        cd_wait(i)
                        load_w(i)

                    pre = jnp.dot(u[pl.ds(pl.multiple_of(m * TM, TM), TM), :], w_buf[a % 2],
                                  preferred_element_type=jnp.float32)
                    cdf = 0.5 * (1.0 + jnp.tanh(0.7978845608028654 * (pre + 0.044715 * (pre * pre * pre))))
                    act = (pre * cdf).astype(jnp.bfloat16)

                    @pl.when(jnp.logical_or(a > 0, m >= 2))
                    def _():
                        for c in h_copies(a, m):
                            c.wait()

                    h_stage[m % 2] = act
                    for c in h_copies(a, m):
                        c.start()

        for m in (0, 1):
            for c in h_copies(NA - 1, m):
                c.wait()

    pl.run_scoped(
        phase_a,
        pltpu.VMEM((ROWS, DIM), jnp.bfloat16),
        pltpu.VMEM((2, DIM, 4 * CA), jnp.bfloat16),
        pltpu.VMEM((2, TM, DIM), jnp.bfloat16),
        pltpu.VMEM((2, TM, 4 * CA), jnp.bfloat16),
        pltpu.VMEM((1, DIM), jnp.float32),
    )

    def phase_b(w_buf, h_buf, x_buf, y_buf, acc_buf):
        early = [(0, 0, 1), (0, 1, 0), (0, 1, 1), (1, 0, 0), (1, 0, 1)]
        late = [(1, 1, 0), (1, 1, 1)]

        def load_pieces(j, pieces, sem):
            slot = j % WS
            for d in pieces:
                wf, wx, wk = who(d)
                r0 = (2 * wx + wk) * F_BLOCK + wf * F_PIECE
                pltpu.make_async_copy(
                    piece_b(j, (wf, wx, wk)),
                    w_buf.at[slot, pl.ds(pl.multiple_of(r0, 32), F_PIECE), :],
                    sem.at[slot]).start()

        def load_early(j):
            c_wait(NA + j)
            load_pieces(j, early, ld_sem)
            r0 = t * F_BLOCK + f * F_PIECE
            pltpu.make_async_copy(
                own_b(j), w_buf.at[j % WS, pl.ds(pl.multiple_of(r0, 32), F_PIECE), :],
                ld_sem.at[j % WS]).start()

        def load_late(j):
            cd_wait(NA + j)
            load_pieces(j, late, ld2_sem)

        def wait_rows(j, n, sem):
            pltpu.make_async_copy(
                g2.at[pl.ds(0, n * F_PIECE), pl.ds(0, CB)],
                w_buf.at[j % WS, pl.ds(0, n * F_PIECE), :], sem.at[j % WS]).wait()

        def hslot(m):
            b = (m + MT - RES) // MT
            return m * (1 - b) + b * (RES + (m + 1) % 2)

        late_cols = [(1 - x) * 2 * F_BLOCK + q * F_BLOCK + (1 - f) * 1664 for q in (0, 1)]
        ranges = {
            "all": [(0, FFN)],
            "early": [(x * 2 * F_BLOCK, 2 * F_BLOCK)] + [
                ((1 - x) * 2 * F_BLOCK + q * F_BLOCK + f * 1792, 1664) for q in (0, 1)],
            "late": [(c0, 1792) for c0 in late_cols],
        }

        def load_h(m, mode):
            rows = pl.ds(pl.multiple_of(m * TM, TM), TM)
            if mode != "late":
                return [pltpu.make_async_copy(
                    hbm_h.at[rows], h_buf.at[hslot(m)], t_sem.at[(m + 1) % 2, 0])]
            return [pltpu.make_async_copy(
                hbm_h.at[rows, pl.ds(pl.multiple_of(c0, 128), 1792)],
                h_buf.at[hslot(m), :, pl.ds(pl.multiple_of(c0, 128), 1792)],
                t_sem.at[(m + 1) % 2, q]) for q, c0 in enumerate(late_cols)]

        def load_x(m, j, n, slot):
            return pltpu.make_async_copy(
                hid.at[pl.ds(pl.multiple_of(m * TM, TM), TM),
                       pl.ds(pl.multiple_of(j * CB, 128), n * CB)],
                x_buf.at[slot, :, pl.ds(0, n * CB)], x_sem.at[slot])

        def store_y(m, j, n, slot):
            return pltpu.make_async_copy(
                y_buf.at[slot, :, pl.ds(0, n * CB)],
                out.at[pl.ds(pl.multiple_of(m * TM, TM), TM),
                       pl.ds(pl.multiple_of(j * CB, 128), n * CB)],
                o_sem.at[slot, 0])

        def compute(j, n, mode, hooks):
            last = mode != "early"
            for q in range(n):
                if mode != "late":
                    wait_rows(j + q, 6, ld_sem)
                if last:
                    wait_rows(j + q, 2, ld2_sem)
            if last:
                load_x(0, j, n, 0).start()

            @pl.loop(0, MT)
            def _(m):
                slot = m % 2

                @pl.when(m == 0)
                def _():
                    for mm in (RES, RES + 1):
                        for c in load_h(mm, mode):
                            c.start()

                if last:
                    pl.when(m + 1 < MT)(lambda: load_x(m + 1, j, n, 1 - slot).start())
                for at, hook in hooks.items():
                    pl.when(m == at)(hook)

                @pl.when(m >= RES)
                def _():
                    for c in load_h(m, mode):
                        c.wait()

                if last:
                    load_x(m, j, n, slot).wait()

                    @pl.when(m >= 2)
                    def _():
                        store_y(m, j, n, slot).wait()

                rows = pl.ds(pl.multiple_of(m * TM, TM), TM)
                for q in range(n):
                    acc = None
                    for c0, size in ranges[mode]:
                        kk = slice(None) if mode == "all" else pl.ds(pl.multiple_of(c0, 128), size)
                        part = jnp.dot(h_buf[hslot(m), :, kk], w_buf[(j + q) % WS, kk, :],
                                       preferred_element_type=jnp.float32)
                        acc = part if acc is None else acc + part
                    if mode == "early":
                        acc_buf[j - (NB - 2), rows, :] = acc
                    else:
                        if mode == "late":
                            acc = acc + acc_buf[j + q - (NB - 2), rows, :]
                        cols = slice(q * CB, (q + 1) * CB)
                        y_buf[slot, :, cols] = (
                            x_buf[slot, :, cols].astype(jnp.float32) + acc).astype(jnp.bfloat16)
                if last:
                    store_y(m, j, n, slot).start()

                @pl.when(jnp.logical_and(m >= RES, m + 2 < MT))
                def _():
                    for c in load_h(m + 2, mode):
                        c.start()

            if last:
                for m in (MT - 2, MT - 1):
                    store_y(m, j, n, m % 2).wait()

        for m in range(RES):
            pltpu.make_async_copy(
                hbm_h.at[pl.ds(m * TM, TM)], h_buf.at[m], t_sem.at[m % 2, m // 2]).start()
        d_point(NA)
        load_early(0)
        load_late(0)
        comm_point(NA + 2)
        d_point(NA + 1)
        for m in range(RES):
            pltpu.make_async_copy(
                hbm_h.at[pl.ds(m * TM, TM)], h_buf.at[m], t_sem.at[m % 2, m // 2]).wait()

        def pair(j):
            load_early(j + 1)
            load_late(j + 1)

            def load():
                load_early(j + 2)
                load_late(j + 2)

            compute(j, 2, "all", {
                3: lambda: comm_point(NA + j + 3),
                6: lambda: d_point(NA + j + 2),
                7: load,
            })

        n_pairs = (NB - 4) // 2

        @pl.loop(0, n_pairs)
        def _(p):
            pair(2 * p)

            @pl.when(p < n_pairs - 1)
            def _():
                comm_point(NA + 2 * p + 4)
                d_point(NA + 2 * p + 3)

        j = NB - 4
        compute(j, 1, "all", {
            0: lambda: load_early(j + 1),
            3: lambda: comm_point(NA + j + 2),
            7: lambda: d_point(NA + j + 1),
        })
        load_late(j + 1)
        compute(j + 1, 1, "all", {
            1: lambda: load_early(j + 2),
            7: lambda: comm_point(NA + j + 3),
        })
        compute(j + 2, 1, "early", {
            2: lambda: load_early(j + 3),
            7: lambda: d_point(NA + j + 2),
        })

        def last_load():
            load_late(j + 3)

        compute(j + 3, 1, "early", {
            1: lambda: load_late(j + 2),
            5: lambda: d_point(NA + j + 3),
            7: last_load,
        })
        compute(j + 2, 2, "late", {})

    pl.run_scoped(
        phase_b,
        pltpu.VMEM((WS, FFN, CB), jnp.bfloat16),
        pltpu.VMEM((RES + 2, TM, FFN), jnp.bfloat16),
        pltpu.VMEM((2, TM, 2 * CB), jnp.bfloat16),
        pltpu.VMEM((2, TM, 2 * CB), jnp.bfloat16),
        pltpu.VMEM((2, ROWS, CB), jnp.float32),
    )

    for kind in range(9):
        rows_a = K_PIECE if kind in (0, 1, 2, 5, 6) else K_PIECE // 2
        pltpu.make_async_copy(w_in.at[pl.ds(0, rows_a)], w_in.at[pl.ds(0, rows_a)],
                              s_sem.at[0, kind]).wait()
        rows_b = F_PIECE if kind in (0, 1, 2, 5, 6) else F_PIECE // 2
        pltpu.make_async_copy(w_out.at[pl.ds(0, rows_b)], w_out.at[pl.ds(0, rows_b)],
                              s_sem.at[1, kind]).wait()


def solution(mesh):
    def local_mlp(hidden, ln_scale, w_in, w_out):
        bf16 = jnp.bfloat16
        y, _, _, _ = pl.pallas_call(
            kernel,
            out_shape=[
                jax.ShapeDtypeStruct((ROWS, DIM), bf16),
                jax.ShapeDtypeStruct((NA, DIM, 4 * CA), bf16),
                jax.ShapeDtypeStruct((FFN, DIM), bf16),
                jax.ShapeDtypeStruct((ROWS, FFN), bf16),
            ],
            in_specs=[pl.BlockSpec(memory_space=pl.ANY)] * 4,
            out_specs=[pl.BlockSpec(memory_space=pl.ANY)] * 4,
            scratch_shapes=[
                pltpu.SemaphoreType.DMA((S,)),
                pltpu.SemaphoreType.DMA((S,)),
                pltpu.SemaphoreType.DMA((S,)),
                pltpu.SemaphoreType.DMA((S,)),
                pltpu.SemaphoreType.DMA((S,)),
                pltpu.SemaphoreType.DMA((S,)),
                pltpu.SemaphoreType.DMA((2, 9)),
                pltpu.SemaphoreType.DMA((WS,)),
                pltpu.SemaphoreType.DMA((WS,)),
                pltpu.SemaphoreType.DMA((2, 2)),
                pltpu.SemaphoreType.DMA((2,)),
                pltpu.SemaphoreType.DMA((2, 4)),
            ],
            compiler_params=pltpu.CompilerParams(
                collective_id=0, has_side_effects=True, vmem_limit_bytes=63 * 2**20),
            name="mlp",
        )(hidden, ln_scale.reshape(1, DIM), w_in, w_out)
        return y

    return jax.shard_map(
        local_mlp,
        mesh=mesh,
        in_specs=(P(("data", "fsdp", "tp"), None), P(None), P("fsdp", "tp"), P(("tp", "fsdp"), None)),
        out_specs=P(("data", "fsdp", "tp"), None),
        check_vma=False,
    )
```

```python
import jax
import jax.numpy as jnp
from jax import lax
from jax.experimental import pallas as pl
from jax.experimental.pallas import tpu as pltpu
from jax.sharding import PartitionSpec as P

LN_EPS = 1e-6
MESH = pl.DeviceIdType.MESH

ROWS, DIM, FFN = 2048, 5120, 13824
K_PIECE, F_BLOCK = 2560, 3456
F_PIECE = 1728
CA, NA = 128, 27
CB, NB = 256, 20
S = NA + NB
LEAD = 2
TM = 256
MT = ROWS // TM
KS = 1152
WS = 3
RES = 3


def kernel(hid, gain, w_in, w_out, out, g1, g2, hbm_h,
           r_x, r_y, r_dx, r_dy, r_c, r_cd, s_sem, ld_sem, ld2_sem, t_sem, x_sem, o_sem):
    f = lax.axis_index("fsdp")
    t = lax.axis_index("tp")
    x, k = t // 2, t % 2
    xn = {"tp": 2 * (1 - x) + k}
    yn = {"fsdp": 1 - f}
    cn = {"tp": 2 * x + 1 - k}
    me = (f, x, k)
    px, py, pd = (f, 1 - x, k), (1 - f, x, k), (1 - f, 1 - x, k)

    def piece_a(i, who, half=None):
        wf, wx, wk = who
        n = K_PIECE if half is None else K_PIECE // 2
        r0 = wf * K_PIECE + (0 if half is None else half * n)
        return g1.at[i, pl.ds(pl.multiple_of(r0, 128), n),
                     pl.ds(pl.multiple_of((2 * wx + wk) * CA, 128), CA)]

    def piece_b(j, who, half=None):
        wf, wx, wk = who
        n = F_PIECE if half is None else F_PIECE // 2
        r0 = (2 * wx + wk) * F_BLOCK + wf * F_PIECE + (0 if half is None else half * n)
        return g2.at[pl.ds(pl.multiple_of(r0, 32), n),
                     pl.ds(pl.multiple_of(j * CB, 128), CB)]

    def own_a(i):
        return w_in.at[:, pl.ds(pl.multiple_of(i * CA, 128), CA)]

    def own_b(j):
        return w_out.at[:, pl.ds(pl.multiple_of(j * CB, 128), CB)]

    def rc(src, dst, kind, ph, recv, dev):
        return pltpu.make_async_remote_copy(
            src, dst, s_sem.at[ph, kind], recv, device_id=dev, device_id_type=MESH)

    phases = ((0, piece_a, own_a, 0, NA), (1, piece_b, own_b, NA, S))

    def each_phase(i, body):
        if isinstance(i, int):
            for ph, piece, own, lo, hi in phases:
                if lo <= i < hi:
                    body(ph, piece, own, i - lo)
            return
        for ph, piece, own, lo, hi in phases:
            pl.when(jnp.logical_and(i >= lo, i < hi))(
                lambda ph=ph, piece=piece, own=own, lo=lo: body(ph, piece, own, i - lo))

    def send_own(i):
        def body(ph, piece, own, n):
            rc(own(n), piece(n, me), 0, ph, r_x.at[i], xn).start()
            rc(own(n), piece(n, me), 1, ph, r_y.at[i], yn).start()
            rc(own(n), piece(n, me), 2, ph, r_c.at[i], cn).start()
        each_phase(i, body)

    def comm_point(i):
        def body(ph, piece, own, n):
            rc(own(n), piece(n, px), 0, ph, r_x.at[i], xn).wait_recv()
            rc(piece(n, px, 0), piece(n, px, 0), 3, ph, r_dy.at[i], yn).start()
            rc(own(n), piece(n, py), 1, ph, r_y.at[i], yn).wait_recv()
            rc(piece(n, py, 1), piece(n, py, 1), 4, ph, r_dx.at[i], xn).start()
            rc(piece(n, px), piece(n, px), 5, ph, r_c.at[i], cn).start()
            rc(piece(n, py), piece(n, py), 6, ph, r_c.at[i], cn).start()
        each_phase(i, body)
        send_own(i + LEAD)

    def d_point(i):
        def body(ph, piece, own, n):
            rc(piece(n, pd, 0), piece(n, pd, 0), 3, ph, r_dy.at[i], yn).wait_recv()
            rc(piece(n, pd, 0), piece(n, pd, 0), 7, ph, r_cd.at[i], cn).start()
            rc(piece(n, pd, 1), piece(n, pd, 1), 4, ph, r_dx.at[i], xn).wait_recv()
            rc(piece(n, pd, 1), piece(n, pd, 1), 8, ph, r_cd.at[i], cn).start()
        each_phase(i, body)

    def c_wait(i):
        def body(ph, piece, own, n):
            whole = (g1.at[n, pl.ds(0, 3 * K_PIECE // 2), pl.ds(0, 2 * CA)] if ph == 0
                     else g2.at[pl.ds(0, 3 * F_PIECE), pl.ds(0, CB)])
            pltpu.make_async_copy(whole, whole, r_c.at[i]).wait()
        each_phase(i, body)

    def cd_wait(i):
        def body(ph, piece, own, n):
            whole = (g1.at[n, pl.ds(0, K_PIECE // 2), pl.ds(0, 2 * CA)] if ph == 0
                     else g2.at[pl.ds(0, F_PIECE), pl.ds(0, CB)])
            pltpu.make_async_copy(whole, whole, r_cd.at[i]).wait()
        each_phase(i, body)

    others = [(a, b, c) for a in (0, 1) for b in (0, 1) for c in (0, 1)][1:]

    def who(d):
        a, b, c = d
        return (1 - f if a else f, 1 - x if b else x, 1 - k if c else k)

    barrier = pltpu.get_barrier_semaphore()
    for nb in (xn, yn, cn):
        pl.semaphore_signal(barrier, inc=1, device_id=nb, device_id_type=MESH)
    pl.semaphore_wait(barrier, 3)
    for i in range(LEAD):
        send_own(i)

    def phase_a(u, w_buf, stage, h_stage, gain_v):
        pltpu.make_async_copy(gain, gain_v, x_sem.at[0]).start()

        def load_rows(m):
            return pltpu.make_async_copy(
                hid.at[pl.ds(m * TM, TM)], stage.at[m % 2], o_sem.at[m % 2, 0])

        load_rows(0).start()
        pltpu.make_async_copy(gain, gain_v, x_sem.at[0]).wait()

        @pl.loop(0, MT)
        def _(m):
            pl.when(m + 1 < MT)(lambda: load_rows(m + 1).start())
            load_rows(m).wait()

            @pl.loop(0, TM // 32)
            def _(r):
                rows = pl.ds(pl.multiple_of(r * 32, 32), 32)
                v = stage[m % 2, rows, :].astype(jnp.float32)
                cen = v - jnp.mean(v, axis=-1, keepdims=True)
                var = jnp.mean(cen * cen, axis=-1, keepdims=True)
                res = cen * lax.rsqrt(var + LN_EPS) * gain_v[...]
                u[pl.ds(pl.multiple_of(m * TM + r * 32, 32), 32), :] = res.astype(jnp.bfloat16)

        def load_w(a):
            slot = a % 2
            for d in others:
                wf, wx, wk = who(d)
                pltpu.make_async_copy(
                    piece_a(a, (wf, wx, wk)),
                    w_buf.at[slot, pl.ds(pl.multiple_of(wf * K_PIECE, 128), K_PIECE),
                             pl.ds(pl.multiple_of((2 * wx + wk) * CA, 128), CA)],
                    ld_sem.at[slot]).start()
            pltpu.make_async_copy(
                own_a(a),
                w_buf.at[slot, pl.ds(pl.multiple_of(f * K_PIECE, 128), K_PIECE),
                         pl.ds(pl.multiple_of(t * CA, 128), CA)],
                ld_sem.at[slot]).start()

        def wait_w(a):
            pltpu.make_async_copy(g1.at[0], w_buf.at[a % 2], ld_sem.at[a % 2]).wait()

        def h_copies(a, m):
            return [pltpu.make_async_copy(
                h_stage.at[m % 2, :, pl.ds(q * CA, CA)],
                hbm_h.at[pl.ds(m * TM, TM), pl.ds(pl.multiple_of(q * F_BLOCK + a * CA, 128), CA)],
                o_sem.at[m % 2, q]) for q in range(4)]

        comm_point(0)

        @pl.loop(0, NA + 1)
        def _(i):
            comm_point(i + 1)
            pl.when(i < NA)(lambda: d_point(i))
            a = i - 1

            @pl.when(i == 0)
            def _():
                c_wait(i)
                cd_wait(i)
                load_w(i)

            @pl.when(i > 0)
            def _():
                wait_w(a)

                @pl.loop(0, MT)
                def _(m):
                    @pl.when(jnp.logical_and(m == 2, i < NA))
                    def _():
                        c_wait(i)
                        cd_wait(i)
                        load_w(i)

                    pre = jnp.dot(u[pl.ds(pl.multiple_of(m * TM, TM), TM), :], w_buf[a % 2],
                                  preferred_element_type=jnp.float32)
                    cdf = 0.5 * (1.0 + jnp.tanh(0.7978845608028654 * (pre + 0.044715 * (pre * pre * pre))))
                    act = (pre * cdf).astype(jnp.bfloat16)

                    @pl.when(jnp.logical_or(a > 0, m >= 2))
                    def _():
                        for c in h_copies(a, m):
                            c.wait()

                    h_stage[m % 2] = act
                    for c in h_copies(a, m):
                        c.start()

        for m in (0, 1):
            for c in h_copies(NA - 1, m):
                c.wait()

    pl.run_scoped(
        phase_a,
        pltpu.VMEM((ROWS, DIM), jnp.bfloat16),
        pltpu.VMEM((2, DIM, 4 * CA), jnp.bfloat16),
        pltpu.VMEM((2, TM, DIM), jnp.bfloat16),
        pltpu.VMEM((2, TM, 4 * CA), jnp.bfloat16),
        pltpu.VMEM((1, DIM), jnp.float32),
    )

    def phase_b(w_buf, h_buf, x_buf, y_buf, acc_buf):
        early = [(0, 0, 1), (0, 1, 0), (0, 1, 1), (1, 0, 0), (1, 0, 1)]
        late = [(1, 1, 0), (1, 1, 1)]

        def load_pieces(j, pieces, sem):
            slot = j % WS
            for d in pieces:
                wf, wx, wk = who(d)
                r0 = (2 * wx + wk) * F_BLOCK + wf * F_PIECE
                pltpu.make_async_copy(
                    piece_b(j, (wf, wx, wk)),
                    w_buf.at[slot, pl.ds(pl.multiple_of(r0, 32), F_PIECE), :],
                    sem.at[slot]).start()

        def load_early(j):
            c_wait(NA + j)
            load_pieces(j, early, ld_sem)
            r0 = t * F_BLOCK + f * F_PIECE
            pltpu.make_async_copy(
                own_b(j), w_buf.at[j % WS, pl.ds(pl.multiple_of(r0, 32), F_PIECE), :],
                ld_sem.at[j % WS]).start()

        def load_late(j):
            cd_wait(NA + j)
            load_pieces(j, late, ld2_sem)

        def wait_rows(j, n, sem):
            pltpu.make_async_copy(
                g2.at[pl.ds(0, n * F_PIECE), pl.ds(0, CB)],
                w_buf.at[j % WS, pl.ds(0, n * F_PIECE), :], sem.at[j % WS]).wait()

        def hslot(m):
            b = (m + MT - RES) // MT
            return m * (1 - b) + b * (RES + (m + 1) % 2)

        late_cols = [(1 - x) * 2 * F_BLOCK + q * F_BLOCK + (1 - f) * 1664 for q in (0, 1)]
        ranges = {
            "all": [(q * KS, KS) for q in range(FFN // KS)],
            "early": [(x * 2 * F_BLOCK + q * KS, KS) for q in range(2 * F_BLOCK // KS)] + [
                ((1 - x) * 2 * F_BLOCK + q * F_BLOCK + f * 1792, 1664) for q in (0, 1)],
            "late": [(c0, 1792) for c0 in late_cols],
        }

        def load_h(m, mode):
            rows = pl.ds(pl.multiple_of(m * TM, TM), TM)
            if mode != "late":
                return [pltpu.make_async_copy(
                    hbm_h.at[rows], h_buf.at[hslot(m)], t_sem.at[(m + 1) % 2, 0])]
            return [pltpu.make_async_copy(
                hbm_h.at[rows, pl.ds(pl.multiple_of(c0, 128), 1792)],
                h_buf.at[hslot(m), :, pl.ds(pl.multiple_of(c0, 128), 1792)],
                t_sem.at[(m + 1) % 2, q]) for q, c0 in enumerate(late_cols)]

        def load_x(m, j, n, slot):
            return pltpu.make_async_copy(
                hid.at[pl.ds(pl.multiple_of(m * TM, TM), TM),
                       pl.ds(pl.multiple_of(j * CB, 128), n * CB)],
                x_buf.at[slot, :, pl.ds(0, n * CB)], x_sem.at[slot])

        def store_y(m, j, n, slot):
            return pltpu.make_async_copy(
                y_buf.at[slot, :, pl.ds(0, n * CB)],
                out.at[pl.ds(pl.multiple_of(m * TM, TM), TM),
                       pl.ds(pl.multiple_of(j * CB, 128), n * CB)],
                o_sem.at[slot, 0])

        def compute(j, n, mode, hooks):
            last = mode != "early"
            for q in range(n):
                if mode != "late":
                    wait_rows(j + q, 6, ld_sem)
                if last:
                    wait_rows(j + q, 2, ld2_sem)
            if last:
                load_x(0, j, n, 0).start()

            @pl.loop(0, MT)
            def _(m):
                slot = m % 2

                @pl.when(m == 0)
                def _():
                    for mm in (RES, RES + 1):
                        for c in load_h(mm, mode):
                            c.start()

                if last:
                    pl.when(m + 1 < MT)(lambda: load_x(m + 1, j, n, 1 - slot).start())
                for at, hook in hooks.items():
                    pl.when(m == at)(hook)

                @pl.when(m >= RES)
                def _():
                    for c in load_h(m, mode):
                        c.wait()

                if last:
                    load_x(m, j, n, slot).wait()

                    @pl.when(m >= 2)
                    def _():
                        store_y(m, j, n, slot).wait()

                rows = pl.ds(pl.multiple_of(m * TM, TM), TM)
                for q in range(n):
                    acc = None
                    for c0, size in ranges[mode]:
                        kk = slice(c0, c0 + size) if mode == "all" else pl.ds(pl.multiple_of(c0, 128), size)
                        part = jnp.dot(h_buf[hslot(m), :, kk], w_buf[(j + q) % WS, kk, :],
                                       preferred_element_type=jnp.float32)
                        acc = part if acc is None else acc + part
                    if mode == "early":
                        acc_buf[j - (NB - 2), rows, :] = acc
                    else:
                        if mode == "late":
                            acc = acc + acc_buf[j + q - (NB - 2), rows, :]
                        cols = slice(q * CB, (q + 1) * CB)
                        y_buf[slot, :, cols] = (
                            x_buf[slot, :, cols].astype(jnp.float32) + acc).astype(jnp.bfloat16)
                if last:
                    store_y(m, j, n, slot).start()

                @pl.when(jnp.logical_and(m >= RES, m + 2 < MT))
                def _():
                    for c in load_h(m + 2, mode):
                        c.start()

            if last:
                for m in (MT - 2, MT - 1):
                    store_y(m, j, n, m % 2).wait()

        for m in range(RES):
            pltpu.make_async_copy(
                hbm_h.at[pl.ds(m * TM, TM)], h_buf.at[m], t_sem.at[m % 2, m // 2]).start()
        d_point(NA)
        load_early(0)
        load_late(0)
        comm_point(NA + 2)
        d_point(NA + 1)
        for m in range(RES):
            pltpu.make_async_copy(
                hbm_h.at[pl.ds(m * TM, TM)], h_buf.at[m], t_sem.at[m % 2, m // 2]).wait()

        def pair(j):
            load_early(j + 1)
            load_late(j + 1)

            def load():
                load_early(j + 2)
                load_late(j + 2)

            compute(j, 2, "all", {
                3: lambda: comm_point(NA + j + 3),
                6: lambda: d_point(NA + j + 2),
                7: load,
            })

        n_pairs = (NB - 4) // 2

        @pl.loop(0, n_pairs)
        def _(p):
            pair(2 * p)

            @pl.when(p < n_pairs - 1)
            def _():
                comm_point(NA + 2 * p + 4)
                d_point(NA + 2 * p + 3)

        j = NB - 4
        compute(j, 1, "all", {
            0: lambda: load_early(j + 1),
            3: lambda: comm_point(NA + j + 2),
            7: lambda: d_point(NA + j + 1),
        })
        load_late(j + 1)
        compute(j + 1, 1, "all", {
            1: lambda: load_early(j + 2),
            7: lambda: comm_point(NA + j + 3),
        })
        compute(j + 2, 1, "early", {
            2: lambda: load_early(j + 3),
            7: lambda: d_point(NA + j + 2),
        })

        def last_load():
            load_late(j + 3)

        compute(j + 3, 1, "early", {
            1: lambda: load_late(j + 2),
            5: lambda: d_point(NA + j + 3),
            7: last_load,
        })
        compute(j + 2, 2, "late", {})

    pl.run_scoped(
        phase_b,
        pltpu.VMEM((WS, FFN, CB), jnp.bfloat16),
        pltpu.VMEM((RES + 2, TM, FFN), jnp.bfloat16),
        pltpu.VMEM((2, TM, 2 * CB), jnp.bfloat16),
        pltpu.VMEM((2, TM, 2 * CB), jnp.bfloat16),
        pltpu.VMEM((2, ROWS, CB), jnp.float32),
    )

    for kind in range(9):
        rows_a = K_PIECE if kind in (0, 1, 2, 5, 6) else K_PIECE // 2
        pltpu.make_async_copy(w_in.at[pl.ds(0, rows_a)], w_in.at[pl.ds(0, rows_a)],
                              s_sem.at[0, kind]).wait()
        rows_b = F_PIECE if kind in (0, 1, 2, 5, 6) else F_PIECE // 2
        pltpu.make_async_copy(w_out.at[pl.ds(0, rows_b)], w_out.at[pl.ds(0, rows_b)],
                              s_sem.at[1, kind]).wait()


def solution(mesh):
    def local_mlp(hidden, ln_scale, w_in, w_out):
        bf16 = jnp.bfloat16
        y, _, _, _ = pl.pallas_call(
            kernel,
            out_shape=[
                jax.ShapeDtypeStruct((ROWS, DIM), bf16),
                jax.ShapeDtypeStruct((NA, DIM, 4 * CA), bf16),
                jax.ShapeDtypeStruct((FFN, DIM), bf16),
                jax.ShapeDtypeStruct((ROWS, FFN), bf16),
            ],
            in_specs=[pl.BlockSpec(memory_space=pl.ANY)] * 4,
            out_specs=[pl.BlockSpec(memory_space=pl.ANY)] * 4,
            scratch_shapes=[
                pltpu.SemaphoreType.DMA((S,)),
                pltpu.SemaphoreType.DMA((S,)),
                pltpu.SemaphoreType.DMA((S,)),
                pltpu.SemaphoreType.DMA((S,)),
                pltpu.SemaphoreType.DMA((S,)),
                pltpu.SemaphoreType.DMA((S,)),
                pltpu.SemaphoreType.DMA((2, 9)),
                pltpu.SemaphoreType.DMA((WS,)),
                pltpu.SemaphoreType.DMA((WS,)),
                pltpu.SemaphoreType.DMA((2, 2)),
                pltpu.SemaphoreType.DMA((2,)),
                pltpu.SemaphoreType.DMA((2, 4)),
            ],
            compiler_params=pltpu.CompilerParams(
                collective_id=0, has_side_effects=True, vmem_limit_bytes=63 * 2**20),
            name="mlp",
        )(hidden, ln_scale.reshape(1, DIM), w_in, w_out)
        return y

    return jax.shard_map(
        local_mlp,
        mesh=mesh,
        in_specs=(P(("data", "fsdp", "tp"), None), P(None), P("fsdp", "tp"), P(("tp", "fsdp"), None)),
        out_specs=P(("data", "fsdp", "tp"), None),
        check_vma=False,
    )
```
